32 devices in a mesh: img: 4 (over x, core), patch: 8 (over z, y).
Axes of the slice: x: 2, y: 2, z: 4, core: 2. Of those that a mesh axis runs over, the one named last changes fastest.
Arguments:
- hidden: bfloat16 [8, 8, 128, 640], P('img', 'patch'), may hold values from -100 to 100
- stale_attn_in: bfloat16 [8, 8, 128, 640], P('img', 'patch'), may hold values from -100 to 100
- stale_conv_in: bfloat16 [8, 8, 128, 640], P('img', 'patch'), may hold values from -6 to 6
- ln_gain: float32 [640], replicated, may hold values from 0.25 to 1.75
- ln_bias: float32 [640], replicated, may hold values from -2 to 2
- w_qkv: bfloat16 [640, 1920], replicated, may hold values from -3 to 3
- w_out: bfloat16 [640, 640], replicated, may hold values from -0.25 to 0.25
- gn_gain: float32 [640], replicated, may hold values from 0.25 to 1.75
- gn_bias: float32 [640], replicated, may hold values from -1.5 to 1.5
- conv_weight: bfloat16 [3, 3, 640, 640], replicated, may hold values from -0.078125 to 0.078125
- conv_bias: float32 [640], replicated, may hold values from -1.5 to 1.5
- time_shift: float32 [8, 640], P('img'), may hold values from -6 to 6
Outputs:
- block_out: bfloat16 [8, 8, 128, 640], P('img', 'patch')
The draws below stay inside these ranges and needn't reach their ends.
All inputs are finite; a program needn't handle non-finite values.
Results may differ from the reference program's by a relative error of at most 0.0075.
The reference program's roundings to bfloat16 on the way count: a program that leaves them out, or rounds other values in their place, can miss the bound.
Values may be sent and summed in bfloat16 or wider, within the bound.
A program may use at most 128 MiB of HBM per device.

```python
import math
import jax
import jax.numpy as jnp
from jax import lax

C = 640
GROUPS = 32
HEAD_DIM = 64
ROWS_DEV = 1
COLS = 128
SAMPLES = 8
ROWS = 8
N_PATCH = 8


def paired_inputs(key):
    base_key = jax.random.fold_in(key, 101)
    subkeys = jax.random.split(base_key, 7)
    full_shape = (SAMPLES, ROWS, COLS, C)
    noise_current = jax.random.truncated_normal(subkeys[0], -4.0, 4.0, full_shape, jnp.float32)
    noise_stale = jax.random.truncated_normal(subkeys[1], -4.0, 4.0, full_shape, jnp.float32)
    pattern = 1.5 * jax.random.truncated_normal(subkeys[6], -4.0, 4.0, (SAMPLES, ROWS, 1, C), jnp.float32)
    row_frac = (jnp.arange(ROWS, dtype=jnp.float32) + 0.5) / ROWS - 0.5
    row_scale = 10.0 ** (row_frac[None, :] + 0.5 * jax.random.uniform(subkeys[2], (SAMPLES, ROWS), jnp.float32) - 0.25)
    col_scale = 2.0 ** (2.0 * jax.random.uniform(subkeys[3], (SAMPLES, COLS), jnp.float32) - 1.0)
    chan_scale = 2.0 ** (2.0 * jax.random.uniform(subkeys[4], (C,), jnp.float32) - 1.0)
    full_scale = row_scale[:, :, None, None] * col_scale[:, None, :, None] * chan_scale
    current = (noise_current + pattern) * full_scale
    stale = (noise_stale + pattern) * full_scale
    current = jnp.clip(current, -96.0, 96.0) * 0.03
    stale = jnp.clip(stale, -96.0, 96.0)
    return (current, stale)


def draw_hidden(key, part):
    return paired_inputs(key)[0].astype(jnp.bfloat16)


def draw_stale_attn_in(key, part):
    return paired_inputs(key)[1].astype(jnp.bfloat16)


def draw_ln_bias(key, part):
    bias_scale = 0.3
    return bias_scale * jax.random.truncated_normal(jax.random.fold_in(key, 303), -4.0, 4.0, (C,), jnp.float32)


def draw_w_qkv(key, part):
    subkeys = jax.random.split(jax.random.fold_in(key, 202), 4)
    query_cols = jax.random.truncated_normal(subkeys[0], -4.0, 4.0, (C, C), jnp.float32) / math.sqrt(C)
    value_cols = jax.random.truncated_normal(subkeys[1], -4.0, 4.0, (C, C), jnp.float32) / math.sqrt(C)
    query_cols = 2.5 * query_cols
    key_cols = jax.random.truncated_normal(subkeys[3], -4.0, 4.0, (C, C), jnp.float32) / math.sqrt(C)
    return jnp.concatenate([query_cols, key_cols, value_cols], 1).astype(jnp.bfloat16)


def block_scale(own_key, extent, pieces, smallest, high):
    factor_of, own = 1.0, jax.random.fold_in(own_key, 6)
    for axis_at, blocks in pieces:
        steps = jnp.exp(jax.random.uniform(jax.random.fold_in(own, axis_at), (blocks,), jnp.float32, smallest / len(pieces), high / len(pieces)))
        factor_of = factor_of * jnp.repeat(steps, extent[axis_at] // blocks).reshape([-1 if axis == axis_at else 1 for axis in range(len(extent))])
    return factor_of


def noise(own_key, shape, scale, reach, cuts=(), kind=jnp.bfloat16):
    drawn = jax.random.normal(own_key, shape, jnp.float32) * scale
    if len(cuts) > 0:
        drawn = block_scale(own_key, shape, cuts, -0.22, 0.18) * drawn
    return jnp.clip(drawn, min=-reach, max=reach).astype(kind)


def setup_inputs(seed: int = 0) -> dict:
    seeds = jax.random.split(jax.random.key(seed), 13)
    return {
        "hidden": draw_hidden(jax.random.fold_in(seeds[12], 71), 0),
        "stale_attn_in": draw_stale_attn_in(jax.random.fold_in(seeds[12], 71), 0),
        "stale_conv_in": noise(seeds[2], (SAMPLES, ROWS, COLS, C), 1.0, 6.0, ((0, 4), (1, 8))),
        "ln_gain": jnp.clip(1.0 + 0.15 * jax.random.normal(seeds[3], (C,), jnp.float32), 0.25, 1.75),
        "ln_bias": draw_ln_bias(jax.random.fold_in(seeds[12], 71), 0),
        "w_qkv": draw_w_qkv(jax.random.fold_in(seeds[12], 71), 0),
        "w_out": noise(seeds[6], (C, C), C ** -0.5, 0.25),
        "gn_gain": jnp.clip(1.0 + 0.15 * jax.random.normal(seeds[7], (C,), jnp.float32), 0.25, 1.75),
        "gn_bias": noise(seeds[8], (C,), 0.3, 1.5, (), jnp.float32),
        "conv_weight": noise(seeds[9], (3, 3, C, C), (9 * C) ** -0.5, 0.078125),
        "conv_bias": noise(seeds[10], (C,), 0.3, 1.5, (), jnp.float32),
        "time_shift": noise(seeds[11], (SAMPLES, C), 1.0, 6.0, ((0, 4),), jnp.float32),
    }


EPSILON = 1e-05

def to_half(values):
    return lax.optimization_barrier(values.astype(jnp.bfloat16))

def layer_norm(values, gain, bias):
    values = values.astype(jnp.float32)
    centre = lax.optimization_barrier(jnp.mean(values, -1, keepdims=True))
    centred = values - centre
    spread = lax.optimization_barrier(jnp.mean(centred * centred, -1, keepdims=True))
    return to_half(centred * lax.rsqrt(spread + EPSILON) * gain + bias)

def reference(hidden, stale_attn_in, stale_conv_in, ln_gain, ln_bias, w_qkv, w_out, gn_gain, gn_bias, conv_weight, conv_bias, time_shift):
    head_count = C // HEAD_DIM
    tokens = ROWS * COLS
    patches = N_PATCH
    per_patch = ROWS_DEV * COLS
    score_scale = HEAD_DIM ** (-0.5)
    fresh_in = layer_norm(hidden, ln_gain, ln_bias).reshape(SAMPLES, tokens, C)
    stale_in = layer_norm(stale_attn_in, ln_gain, ln_bias).reshape(SAMPLES, tokens, C)

    def split_heads(values):
        return values.reshape(patches, per_patch, head_count, HEAD_DIM).transpose(2, 0, 1, 3)

    def one_head(head_parts):
        queries, fresh_keys, fresh_values, stale_keys, stale_values = head_parts
        queries = queries.astype(jnp.float32)
        remote = jnp.einsum('pqd,rkd->pqrk', queries, stale_keys.astype(jnp.float32)) * score_scale
        local_scores = jnp.einsum('pqd,pkd->pqk', queries, fresh_keys.astype(jnp.float32)) * score_scale
        same_patch = jnp.eye(patches, dtype=bool)[:, None, :, None]
        remote = jnp.where(same_patch, -jnp.inf, remote)
        row_max = jnp.maximum(lax.optimization_barrier(jnp.max(remote, axis=(2, 3))), lax.optimization_barrier(jnp.max(local_scores, -1)))
        remote_weights = jnp.exp(remote - row_max[:, :, None, None])
        local_weights = jnp.exp(local_scores - row_max[:, :, None])
        weight_sum = lax.optimization_barrier(jnp.sum(remote_weights, axis=(2, 3))) + lax.optimization_barrier(jnp.sum(local_weights, -1))
        gathered = jnp.einsum('pqrk,rkd->pqd', to_half(remote_weights).astype(jnp.float32), stale_values.astype(jnp.float32))
        gathered = gathered + jnp.einsum('pqk,pkd->pqd', to_half(local_weights).astype(jnp.float32), fresh_values.astype(jnp.float32))
        return gathered / weight_sum[:, :, None]

    def attend_sample(operands):
        fresh_rows, stale_rows = operands
        projected = to_half(jnp.dot(fresh_rows, w_qkv, preferred_element_type=jnp.float32))
        stale_pairs = to_half(jnp.dot(stale_rows, w_qkv[:, C:], preferred_element_type=jnp.float32))
        head_parts = (split_heads(projected[:, :C]), split_heads(projected[:, C:2 * C]), split_heads(projected[:, 2 * C:]), split_heads(stale_pairs[:, :C]), split_heads(stale_pairs[:, C:]))
        per_head = lax.map(one_head, head_parts)
        attended = to_half(per_head.transpose(1, 2, 0, 3).reshape(tokens, C))
        return jnp.dot(attended, w_out, preferred_element_type=jnp.float32)
    attention_out = lax.map(attend_sample, (fresh_in, stale_in))
    residual = to_half(hidden.reshape(SAMPLES, tokens, C).astype(jnp.float32) + attention_out)
    grouped = residual.astype(jnp.float32).reshape(SAMPLES, tokens, GROUPS, C // GROUPS)
    group_mean = lax.optimization_barrier(jnp.mean(grouped, axis=(1, 3), keepdims=True))
    centred = grouped - group_mean
    group_var = lax.optimization_barrier(jnp.mean(centred * centred, axis=(1, 3), keepdims=True))
    normalized = (centred * lax.rsqrt(group_var + EPSILON)).reshape(SAMPLES, tokens, C)
    activated = to_half(jax.nn.silu(normalized * gn_gain + gn_bias)).reshape(SAMPLES, ROWS, COLS, C)

    def convolve(operands):
        fresh_rows, stale_rows = operands
        fresh_patch = fresh_rows.reshape(patches, ROWS_DEV, COLS, C)
        stale_patch = stale_rows.reshape(patches, ROWS_DEV, COLS, C)
        zero_rim = jnp.zeros((1, 1, COLS, C), jnp.bfloat16)
        rim_above = jnp.concatenate([zero_rim, stale_patch[:-1, ROWS_DEV - 1:]], 0)
        rim_below = jnp.concatenate([stale_patch[1:, :1], zero_rim], 0)
        framed = jnp.concatenate([rim_above, fresh_patch, rim_below], 1)
        framed = jnp.pad(framed, ((0, 0), (0, 0), (1, 1), (0, 0)))
        summed = jnp.zeros((patches * ROWS_DEV * COLS, C), jnp.float32)
        for tap_row in range(3):
            for tap_col in range(3):
                window = framed[:, tap_row:tap_row + ROWS_DEV, tap_col:tap_col + COLS, :].reshape(-1, C)
                summed = summed + jnp.dot(window, conv_weight[tap_row, tap_col], preferred_element_type=jnp.float32)
        return summed.reshape(ROWS, COLS, C)
    convolved = lax.map(convolve, (activated, stale_conv_in))
    summed_out = convolved + conv_bias + time_shift[:, None, None, :] + residual.astype(jnp.float32).reshape(SAMPLES, ROWS, COLS, C)
    return summed_out.astype(jnp.bfloat16)
```

```python
import functools

import jax
import jax.numpy as jnp
from jax import lax
from jax.experimental import pallas as pl
from jax.experimental.pallas import tpu as pltpu
from jax.sharding import PartitionSpec as P

GROUPS = 32
HEAD_DIM = 64
EPSILON = 1e-05
PARTS = 2
EDGE_STEP = 0
PASS_STEP = 2
MESH = pl.DeviceIdType.MESH
F32 = jnp.float32
BF16 = jnp.bfloat16


def layer_norm(values, gain, bias):
    values = values.astype(F32)
    centre = jnp.mean(values, -1, keepdims=True)
    centred = values - centre
    spread = jnp.mean(centred * centred, -1, keepdims=True)
    return (centred * lax.rsqrt(spread + EPSILON) * gain + bias).astype(BF16)


def dot(a, b):
    return jnp.dot(a, b, preferred_element_type=F32)


def split_dot(a, b):
    high = a.astype(BF16)
    rest = a - high.astype(F32)
    mid = rest.astype(BF16)
    low = (rest - mid.astype(F32)).astype(BF16)
    return dot(high, b) + dot(mid, b) + dot(low, b)


def kernel(
    n,
    hidden,
    stale_attn,
    stale_conv,
    ln_gain_hbm,
    ln_bias_hbm,
    w_qkv_hbm,
    w_out_hbm,
    gn_gain_hbm,
    gn_bias_hbm,
    conv_w_hbm,
    conv_bias_hbm,
    time_shift,
    out,
    ln_gain,
    ln_bias,
    gn_gain,
    gn_bias,
    conv_bias,
    vector_sem,
    w_qkv,
    w_out,
    conv_w,
    blocks,
    edges,
    w_vt,
    q_diag,
    maxima,
    sums,
    accum,
    same_group,
    conv_acc,
    stats,
    weight_sem,
    gather_send,
    gather_recv,
    edge_send,
    edge_recv,
    stat_send,
    stat_recv,
):
    samples, _, cols, channels = hidden.shape
    tokens = samples * cols
    pairs = channels // (2 * HEAD_DIM)
    wide = 2 * cols
    group_size = channels // GROUPS
    side = 2
    length = n // side
    me = lax.axis_index("patch")
    z = me // side
    y = me % side

    load_qkv = pltpu.make_async_copy(w_qkv_hbm, w_qkv, weight_sem.at[0])
    load_out = pltpu.make_async_copy(w_out_hbm, w_out, weight_sem.at[1])
    load_conv = pltpu.make_async_copy(conv_w_hbm, conv_w, weight_sem.at[2])
    vectors = [
        pltpu.make_async_copy(source, target, vector_sem.at[i])
        for i, (source, target) in enumerate(
            (
                (ln_gain_hbm, ln_gain),
                (ln_bias_hbm, ln_bias),
                (gn_gain_hbm, gn_gain),
                (gn_bias_hbm, gn_bias),
                (conv_bias_hbm, conv_bias),
            )
        )
    ]
    for load in vectors:
        load.start()
    load_qkv.start()
    load_out.start()
    load_conv.start()

    barrier = pltpu.get_barrier_semaphore()
    for step in range(1, n):
        pl.semaphore_signal(
            barrier, inc=1, device_id={"patch": lax.rem(me + step, n)}, device_id_type=MESH
        )
    for load in vectors:
        load.wait()
    parts = blocks.shape[1]
    normed = layer_norm(stale_attn[:, 0], ln_gain[...], ln_bias[...])
    blocks[me] = normed.reshape(parts, tokens // parts, channels)
    pl.semaphore_wait(barrier, n - 1)

    def block_copy(way, source, part, target):
        return pltpu.make_async_remote_copy(
            src_ref=blocks.at[source, part],
            dst_ref=blocks.at[source, part],
            send_sem=gather_send.at[way, source, part],
            recv_sem=gather_recv.at[source, part],
            device_id={"patch": target},
            device_id_type=MESH,
        )

    def spread(source_z, source_y, part, act):
        source = source_z * side + source_y
        late = part >= parts // 2
        own_column = source_y == y
        gap = jnp.abs(source_z - z)
        at_end = (z == 0) | (z == length - 1)
        across = own_column & ((gap != 1) if late else ((gap != 1) | at_end))
        pl.when(across)(lambda: act(block_copy(2, source, part, z * side + (1 - y))))
        up = own_column & (source_z <= z) & (z < length - 1)
        down = own_column & (source_z >= z) & (z > 0)
        pl.when(up)(lambda: act(block_copy(0, source, part, me + side)))
        pl.when(down)(lambda: act(block_copy(1, source, part, me - side)))
        beside = (source_y != y) & (gap == 0)
        turn_up = beside & (z < (length - 1 if late else length - 2))
        turn_down = beside & (z > (0 if late else 1))
        pl.when(turn_up)(lambda: act(block_copy(3, source, part, me + side)))
        pl.when(turn_down)(lambda: act(block_copy(4, source, part, me - side)))

    def arrival(k):
        j = (k + 1) // 2
        other = 1 - (k % 2)
        near = jnp.minimum(z, length - 1 - z)
        toward = jnp.where(z * 2 < length, 1, -1)
        both = j <= 2 * near
        step = jnp.where(both, (j + 1) // 2, j - near)
        sign = jnp.where(both, jnp.where(j % 2 == 1, toward, -toward), toward)
        return z + jnp.where(j == 0, 0, step * sign), jnp.where(other == 1, 1 - y, y)

    for part in range(parts):
        spread(z, y, part, lambda copy: copy.start())

    def edge_copy(hop):
        return pltpu.make_async_remote_copy(
            src_ref=stale_conv.at[:, 0] if hop == 0 else edges.at[1 - y],
            dst_ref=edges.at[y],
            send_sem=edge_send.at[hop],
            recv_sem=edge_recv.at[y],
            device_id={"patch": z * side + (1 - y) if hop == 0 else me + side * (1 - 2 * y)},
            device_id_type=MESH,
        )

    def edge_wait(slot):
        pltpu.make_async_remote_copy(
            src_ref=edges.at[slot],
            dst_ref=edges.at[slot],
            send_sem=edge_send.at[0],
            recv_sem=edge_recv.at[slot],
            device_id={"patch": z * side + (1 - y)},
            device_id_type=MESH,
        ).wait_recv()

    below_exists = z < length - 1
    above_exists = z > 0
    hands_on = ((y == 0) & below_exists) | ((y == 1) & above_exists)
    is_handed = ((y == 0) & above_exists) | ((y == 1) & below_exists)

    fresh = layer_norm(hidden[:, 0], ln_gain[...], ln_bias[...]).reshape(tokens, channels)
    load_qkv.wait()
    queries = dot(fresh, w_qkv[:, :channels]).astype(BF16).astype(F32) * HEAD_DIM ** (-0.5)
    q_t = queries.T.astype(BF16)
    q_diag[...] = jnp.zeros_like(q_diag)
    for sample in range(samples):
        for pair in range(pairs):
            for half in range(2):
                row = (2 * pair + half) * HEAD_DIM
                q_diag[
                    sample, pair, half * HEAD_DIM : (half + 1) * HEAD_DIM, half * cols : (half + 1) * cols
                ] = q_t[row : row + HEAD_DIM, sample * cols : (sample + 1) * cols]
    w_vt[...] = w_qkv[:, 2 * channels :].astype(F32).T.astype(BF16)
    channel_row = lax.broadcasted_iota(jnp.int32, (channels, channels), 0) // group_size
    channel_col = lax.broadcasted_iota(jnp.int32, (channels, channels), 1) // group_size
    same_group[...] = jnp.where(channel_row == channel_col, 1.0, 0.0).astype(BF16)

    def absorb(groups, first):
        rows = jnp.concatenate([g[s] for s in range(samples) for g in groups], 0)
        width = len(groups) * cols
        keys = dot(rows, w_qkv[:, channels : 2 * channels]).astype(BF16)
        values_t = lax.dot_general(
            w_vt[...], rows, (((1,), (1,)), ((), ())), preferred_element_type=F32
        ).astype(BF16)
        for sample in range(samples):
            span = slice(sample * width, (sample + 1) * width)
            for pair in range(pairs):
                scores = dot(
                    keys[span, pair * 2 * HEAD_DIM : (pair + 1) * 2 * HEAD_DIM], q_diag[sample, pair]
                )
                new_max = jnp.max(scores, 0, keepdims=True)
                if not first:
                    old_max = maxima[sample, pair : pair + 1]
                    new_max = jnp.maximum(old_max, new_max)
                    rescale = jnp.exp(old_max - new_max)
                weights = jnp.exp(scores - new_max)
                total = jnp.sum(weights, 0, keepdims=True)
                if not first:
                    total = total + sums[sample, pair : pair + 1] * rescale
                maxima[sample, pair : pair + 1] = new_max
                sums[sample, pair : pair + 1] = total
                weights = weights.astype(BF16)
                for half in range(2):
                    row = (2 * pair + half) * HEAD_DIM
                    lanes = slice(half * cols, (half + 1) * cols)
                    part = dot(values_t[row : row + HEAD_DIM, span], weights[:, lanes])
                    if not first:
                        part = part + accum[sample, row : row + HEAD_DIM] * rescale[:, lanes]
                    accum[sample, row : row + HEAD_DIM] = part

    absorb([fresh.reshape(samples, cols, channels)], True)

    def receive(k):
        source_z, source_y = arrival(k)
        source = source_z * side + source_y
        for part in range(parts):
            block_copy(0, source, part, source).wait_recv()
            spread(source_z, source_y, part, lambda copy: copy.start())
        return source

    def block(source):
        return blocks[source].reshape(samples, cols, channels)

    def pass_edges():
        edge_wait(1 - y)
        pl.when(hands_on)(lambda: edge_copy(1).start())

    def step(j, carry):
        first, second = receive(2 * j), receive(2 * j + 1)
        pl.when(j == EDGE_STEP)(lambda: edge_copy(0).start())
        pl.when(j == PASS_STEP)(pass_edges)
        absorb([block(first), block(second)], False)
        return carry

    lax.fori_loop(0, (n - 1) // 2, step, 0)
    if (n - 1) % 2 == 1:
        absorb([block(receive(n - 2))], False)

    for sample in range(samples):
        for head in range(2 * pairs):
            row = head * HEAD_DIM
            total = sums[sample, head // 2 : head // 2 + 1, (head % 2) * cols : (head % 2 + 1) * cols]
            accum[sample, row : row + HEAD_DIM] = accum[sample, row : row + HEAD_DIM] / total
    attended = jnp.concatenate([accum[s].T for s in range(samples)], 0).astype(BF16)
    load_out.wait()
    residual = hidden[:, 0].reshape(tokens, channels).astype(F32) + dot(attended, w_out[...])
    residual = residual.astype(BF16).astype(F32).reshape(samples, cols, channels)

    sum_rows = jnp.concatenate([jnp.sum(residual[s], 0, keepdims=True) for s in range(samples)], 0)
    cells = cols * group_size
    local_mean = split_dot(sum_rows, same_group[...]) / cells
    centred = residual - local_mean[:, None, :]
    square_rows = jnp.concatenate(
        [jnp.sum(centred[s] * centred[s], 0, keepdims=True) for s in range(samples)], 0
    )
    local_square = split_dot(square_rows, same_group[...])
    stats[me, :samples] = local_mean
    stats[me, samples:] = local_square

    def stat_copy(distance):
        return pltpu.make_async_remote_copy(
            src_ref=stats.at[me],
            dst_ref=stats.at[me],
            send_sem=stat_send.at[distance],
            recv_sem=stat_recv.at[me],
            device_id={"patch": lax.rem(me + distance, n)},
            device_id_type=MESH,
        )

    for distance in range(1, n):
        stat_copy(distance).start()

    @pl.when(me == 0)
    def _():
        edges[0] = jnp.zeros_like(edges[0])

    @pl.when(me == n - 1)
    def _():
        edges[1] = jnp.zeros_like(edges[1])

    pl.when(is_handed)(lambda: edge_wait(y))
    load_conv.wait()
    above = edges[0].reshape(tokens, channels)
    below = edges[1].reshape(tokens, channels)
    for tap in range(3):
        conv_acc[tap] = dot(above, conv_w[0, tap]) + dot(below, conv_w[2, tap])

    for distance in range(1, n):
        source = lax.rem(me + distance, n)
        pltpu.make_async_remote_copy(
            src_ref=stats.at[source],
            dst_ref=stats.at[source],
            send_sem=stat_send.at[distance],
            recv_sem=stat_recv.at[source],
            device_id={"patch": source},
            device_id_type=MESH,
        ).wait_recv()
    every = stats[...]
    group_mean = jnp.mean(every[:, :samples], 0)
    shift = every[:, :samples] - group_mean[None]
    group_var = (jnp.sum(every[:, samples:], 0) + cells * jnp.sum(shift * shift, 0)) / (cells * n)
    scale = lax.rsqrt(group_var + EPSILON)
    pre = (residual - group_mean[:, None, :]) * scale[:, None, :] * gn_gain[...] + gn_bias[...]
    activated = (pre / (1.0 + jnp.exp(-pre))).astype(BF16).reshape(tokens, channels)

    column = lax.broadcasted_iota(jnp.int32, (tokens, 1), 0) % cols
    total = conv_acc[1] + dot(activated, conv_w[1, 1])
    left = pltpu.roll(conv_acc[0] + dot(activated, conv_w[1, 0]), 1, 0)
    total = total + jnp.where(column == 0, 0.0, left)
    right = pltpu.roll(conv_acc[2] + dot(activated, conv_w[1, 2]), tokens - 1, 0)
    total = total + jnp.where(column == cols - 1, 0.0, right)
    total = total.reshape(samples, cols, channels) + conv_bias[...]
    for sample in range(samples):
        out[sample, 0] = (
            total[sample] + time_shift[sample : sample + 1] + residual[sample]
        ).astype(BF16)

    for part in range(parts):
        spread(z, y, part, lambda copy: copy.wait_send())

    def drain(k, carry):
        source_z, source_y = arrival(k)
        for part in range(parts):
            spread(source_z, source_y, part, lambda copy: copy.wait_send())
        return carry

    lax.fori_loop(0, n - 1, drain, 0)
    edge_copy(0).wait_send()
    pl.when(hands_on)(lambda: edge_copy(1).wait_send())
    for distance in range(1, n):
        stat_copy(distance).wait_send()


def shards(n, *arrays):
    (hidden, stale_attn, stale_conv, ln_gain, ln_bias, w_qkv, w_out) = arrays[:7]
    (gn_gain, gn_bias, conv_w, conv_bias, time_shift) = arrays[7:]
    samples, rows_dev, cols, channels = hidden.shape
    assert rows_dev == 1 and n % 2 == 0, "unsupported split"
    tokens = samples * cols
    parts = PARTS * samples
    pairs = channels // (2 * HEAD_DIM)
    vmem = pl.BlockSpec(memory_space=pltpu.VMEM)
    hbm = pl.BlockSpec(memory_space=pl.ANY)
    dma = pltpu.SemaphoreType.DMA
    return pl.pallas_call(
        functools.partial(kernel, n),
        out_shape=jax.ShapeDtypeStruct(hidden.shape, BF16),
        in_specs=[vmem] * 3 + [hbm] * 8 + [vmem],
        out_specs=vmem,
        scratch_shapes=[pltpu.VMEM((channels,), F32)] * 5
        + [
            dma((5,)),
            pltpu.VMEM(w_qkv.shape, BF16),
            pltpu.VMEM(w_out.shape, BF16),
            pltpu.VMEM(conv_w.shape, BF16),
            pltpu.VMEM((n, parts, tokens // parts, channels), BF16),
            pltpu.VMEM((2, samples, cols, channels), BF16),
            pltpu.VMEM((channels, channels), BF16),
            pltpu.VMEM((samples, pairs, 2 * HEAD_DIM, 2 * cols), BF16),
            pltpu.VMEM((samples, pairs, 2 * cols), F32),
            pltpu.VMEM((samples, pairs, 2 * cols), F32),
            pltpu.VMEM((samples, channels, cols), F32),
            pltpu.VMEM((channels, channels), BF16),
            pltpu.VMEM((3, tokens, channels), F32),
            pltpu.VMEM((n, 2 * samples, channels), F32),
            dma((3,)),
            dma((5, n, parts)),
            dma((n, parts)),
            dma((2,)),
            dma((2,)),
            dma((n,)),
            dma((n,)),
        ],
        compiler_params=pltpu.CompilerParams(
            collective_id=0, has_side_effects=True, vmem_limit_bytes=56 * 2**20
        ),
        name="section",
    )(
        hidden,
        stale_attn,
        stale_conv,
        ln_gain,
        ln_bias,
        w_qkv,
        w_out,
        gn_gain,
        gn_bias,
        conv_w,
        conv_bias,
        time_shift,
    )


def solution(mesh):
    wide = P("img", "patch", None, None)
    in_specs = (wide, wide, wide) + (P(),) * 8 + (P("img", None),)
    body = functools.partial(shards, mesh.shape["patch"])
    return jax.shard_map(body, mesh=mesh, in_specs=in_specs, out_specs=wide, check_vma=False)
```
